32 devices in a mesh: mem: 8 (over y, x, core), patch: 4 (over z).
Axes of the slice: x: 2, y: 2, z: 4, core: 2. Of those that a mesh axis runs over, the one named last changes fastest.
Arguments:
- state: bfloat16 [1024, 16384], P('mem', 'patch'), may hold values from -6 to 6
- obs_ens: bfloat16 [1024, 8192], P('mem', 'patch'), may hold values from -6 to 6
- obs_values: float32 [8192], P('patch'), may hold values from -8 to 8
- obs_weight: float32 [8192], P('patch'), may hold values from 0.2 to 5
- counts: int32 [32], P('patch'), may hold values from 32 to 256
Outputs:
- analysis: bfloat16 [1024, 16384], P('mem', 'patch')
The draws below stay inside these ranges and needn't reach their ends.
Inputs may be any that keep to these rules, and one draw needn't show every extreme that they name: Region r uses the first counts[r] of its 256 observations.
All inputs are finite; a program needn't handle non-finite values. Where the reference program divides by a largest or mean magnitude, that divisor is 1e-20 or more.
Results may differ from the reference program's by a relative error of at most 0.0047.
Values may be sent and summed in bfloat16 or wider, within the bound.
A program may use at most 64 MiB of HBM per device.

```python
import math
import jax
import jax.numpy as jnp
from jax import lax

MEMBERS = 1024
REGION_ROWS = 512
OBS_OWN = 256
DEGREE = 7
REGIONS_PATCH = 8
REGIONS = 32
NROWS = 16384
NOBS = 8192


def set_ends(array, stream_key, low, high):
    longest = array.shape.index(max(array.shape))
    spots = []
    for shift in (0, 1):
        where = [jax.random.randint(jax.random.fold_in(stream_key, axis), (), 0, length) for axis, length in enumerate(array.shape)]
        where[longest] = (where[longest] + shift) % array.shape[longest]
        spots.append(tuple(where))
    return array.at[spots[0]].set(low).at[spots[1]].set(high)


def level_of(key, extent, cuts, least, top_value):
    loudness = 1.0
    for axis_at, blocks in cuts:
        heights = jax.random.uniform(jax.random.fold_in(jax.random.fold_in(key, 6), axis_at), (blocks,), jnp.float32, least / len(cuts), top_value / len(cuts))
        loudness = loudness * jnp.repeat(jnp.exp(heights), extent[axis_at] // blocks).reshape((-1,) + (1,) * (len(extent) - 1 - axis_at))
    return loudness


def bell_draw(own_key, dims, width, reach, shards=(), kind=jnp.bfloat16):
    array = jax.random.normal(own_key, dims, jnp.float32) * width
    if len(shards) > 0:
        array = level_of(own_key, dims, shards, -0.22, 0.18) * array
    return jnp.clip(array, min=-reach, max=reach).astype(kind)


def setup_inputs(seed: int = 0) -> dict:
    arg_keys = jax.random.split(jax.random.key(seed), 6)
    return {
        "state": bell_draw(arg_keys[0], (MEMBERS, NROWS), 1.0, 6.0, ((0, 8), (1, 4))),
        "obs_ens": bell_draw(arg_keys[1], (MEMBERS, NOBS), 1.0, 6.0, ((0, 8), (1, 4))),
        "obs_values": bell_draw(arg_keys[2], (NOBS,), 1.5, 8.0, ((0, 4),), jnp.float32),
        "obs_weight": jnp.clip(jnp.exp(math.log(5.0) - 3.218876 * jax.random.uniform(arg_keys[3], (NOBS,), jnp.float32) ** level_of(arg_keys[3], (NOBS,), ((0, 4),), -0.2, 0.2)), 0.2, 5.0),
        "counts": set_ends(jax.random.randint(arg_keys[4], (REGIONS,), OBS_OWN // 8, OBS_OWN + 1), jax.random.fold_in(arg_keys[4], 1), OBS_OWN // 8, OBS_OWN).astype(jnp.int32),
    }


def root_curve(values):
    lifted = jnp.sqrt(1.0 + values)
    return -1.0 / (lifted * (1.0 + lifted))

def inverse_curve(values):
    return 1.0 / (1.0 + values)

def chebyshev(upper, curve):
    number = DEGREE + 1
    theta = (jnp.arange(number, dtype=jnp.float32) + 0.5) * (math.pi / number)
    nodes = upper * (jnp.cos(theta) + 1.0) * 0.5
    samples = curve(nodes)
    orders = jnp.arange(number, dtype=jnp.float32)
    table = jnp.cos(orders[:, None] * theta[None, :])
    coefs = 2.0 / number * lax.optimization_barrier(jnp.sum(table * samples[None, :], axis=1))
    return coefs * jnp.where(orders == 0.0, 0.5, 1.0)

def clenshaw(block, matrix, coefs):
    nearer = coefs[DEGREE] * block
    farther = jnp.zeros_like(block)
    for order in range(DEGREE - 1, 0, -1):
        current = coefs[order] * block + 2.0 * jnp.dot(nearer, matrix, precision=lax.Precision.HIGHEST) - farther
        farther, nearer = (nearer, current)
    return coefs[0] * block + jnp.dot(nearer, matrix, precision=lax.Precision.HIGHEST) - farther

def perturb_obs(obs_block, values, weights, count):
    full = obs_block.astype(jnp.float32)
    centre = lax.optimization_barrier(jnp.mean(full, axis=0))
    mask = (jnp.arange(values.shape[0], dtype=jnp.int32) < count).astype(jnp.float32)
    root = jnp.sqrt(weights * mask)
    gains = ((full - centre[None, :]) * root[None, :]).astype(jnp.bfloat16)
    innov = (root * (values - centre)).astype(jnp.bfloat16)
    return jnp.concatenate([gains, innov[None, :]], axis=0)

def transform(region_state, stacked):
    gains = stacked[:-1]
    innov = stacked[-1].astype(jnp.float32)
    members = gains.shape[0]
    normal = jnp.dot(gains.T, gains, preferred_element_type=jnp.float32) / (members - 1)
    upper = jnp.max(lax.optimization_barrier(jnp.sum(jnp.abs(normal), axis=1))) + 1e-06
    shifted = normal * (2.0 / upper) - jnp.eye(normal.shape[0], dtype=jnp.float32)
    full = region_state.astype(jnp.float32)
    centre = lax.optimization_barrier(jnp.mean(full, axis=0))
    spread = (full - centre[None, :]).astype(jnp.bfloat16)
    product = jnp.dot(spread.T, gains, preferred_element_type=jnp.float32)
    mixed = clenshaw(product, shifted, chebyshev(upper, root_curve)).astype(jnp.bfloat16)
    mean_weights = clenshaw(innov[None, :], shifted, chebyshev(upper, inverse_curve))[0]
    mean_shift = jnp.dot(product, mean_weights, precision=lax.Precision.HIGHEST) / (members - 1)
    update = jnp.dot(gains, mixed.T, preferred_element_type=jnp.float32) / (members - 1)
    return (full + mean_shift[None, :] + update).astype(jnp.bfloat16)

def reference(state, obs_ens, obs_values, obs_weight, counts):
    order = jnp.arange(REGIONS, dtype=jnp.int32)

    def own_part(region):
        start = region * OBS_OWN
        block = lax.dynamic_slice_in_dim(obs_ens, start, OBS_OWN, 1)
        values = lax.dynamic_slice_in_dim(obs_values, start, OBS_OWN, 0)
        weights = lax.dynamic_slice_in_dim(obs_weight, start, OBS_OWN, 0)
        return perturb_obs(block, values, weights, counts[region])
    stacked = lax.map(own_part, order)
    half = OBS_OWN // 2

    def one_region(region):
        left = stacked[(region - REGIONS_PATCH) % REGIONS][:, OBS_OWN - half:]
        right = stacked[(region + REGIONS_PATCH) % REGIONS][:, :half]
        joined = jnp.concatenate([left, stacked[region], right], axis=1)
        block = lax.dynamic_slice_in_dim(state, region * REGION_ROWS, REGION_ROWS, 1)
        return transform(block, joined)
    result = lax.map(one_region, order)
    return jnp.transpose(result, (1, 0, 2)).reshape(MEMBERS, NROWS)
```

```python
import functools
import math

import jax
import jax.numpy as jnp
import numpy as np
from jax import lax
from jax.experimental import pallas as pl
from jax.experimental.pallas import tpu as pltpu
from jax.sharding import PartitionSpec as P

DEGREE = 7
MESH = pl.DeviceIdType.MESH
PAD = 16


def functionals():
    number = DEGREE + 1
    theta = (np.arange(number) + 0.5) * (math.pi / number)
    rows = 2.0 / number * np.cos(np.arange(number)[:, None] * theta[None, :])
    rows[0] *= 0.5
    a = rows
    signs = np.where(np.arange(number) % 2 == 0, 1.0, -1.0)
    table = np.stack(
        [
            (signs[:, None] * a).sum(0),
            a[1] - a[7] + 2 * a[5],
            a[2] + a[6],
            a[3] - a[5] + 2 * a[7],
            a[4] - 2 * a[5] + 2 * a[6] - 2 * a[7],
            2 * a[5],
            2 * a[6],
            2 * a[7],
        ]
    )
    return (np.cos(theta) + 1.0) * 0.5, table


def flipped(index, step, count):
    bit = 1
    while bit < count:
        if step & bit:
            index = index + bit - 2 * bit * (lax.rem(index // bit, 2))
        bit *= 2
    return index


def split(row):
    high = row.astype(jnp.bfloat16)
    low = (row - high.astype(jnp.float32)).astype(jnp.bfloat16)
    return high, low


def row_times(row, matrix):
    high, low = split(row)
    k = row.shape[1]
    pick = lax.broadcasted_iota(jnp.int32, (PAD, k), 0)
    both = jnp.where(
        pick == 0,
        jnp.broadcast_to(high.astype(jnp.float32), (PAD, k)),
        jnp.where(pick == 1, jnp.broadcast_to(low.astype(jnp.float32), (PAD, k)), 0.0),
    ).astype(jnp.bfloat16)
    return jnp.sum(dot(both, matrix), axis=0, keepdims=True)


def dot(left, right):
    return jnp.dot(left, right, preferred_element_type=jnp.float32)


def kernel(
    n, npatch,
    aux_ref, obs_hbm, state_hbm, out_hbm,
    obs_v, state_v, gain, gain_t, pt, out_v,
    d1, d2, d3, d4,
    obs_ss, obs_rs, st_ss, st_rs, edge_ss, edge_rs, out_ss, out_rs, loc,
):
    me = lax.axis_index("mem")
    patch = lax.axis_index("patch")
    rows = obs_hbm.shape[0]
    own = obs_v.shape[1]
    half = own // 2
    width = state_v.shape[1]
    members = n * rows
    nobs = 2 * own
    up = lax.rem(patch + 1, npatch)
    down = lax.rem(patch + npatch - 1, npatch)

    def cols(index, size):
        return pl.ds(pl.multiple_of(index * size, size), size)

    group = max(1, 256 // rows)
    groups = n // group
    order = list(range(groups - 1, 0, -1))
    steps = [s * group + i for i in range(group) for s in order] + list(range(1, group))

    barrier = pltpu.get_barrier_semaphore()
    for s in range(1, n):
        pl.semaphore_signal(barrier, inc=1, device_id=(flipped(me, s, n), patch), device_id_type=MESH)
    for p in (up, down):
        pl.semaphore_signal(barrier, inc=1, device_id=(me, p), device_id_type=MESH)
    own_obs = pltpu.make_async_copy(obs_hbm.at[:, cols(me, own)], obs_v.at[cols(me, rows), :], loc.at[0])
    own_obs.start()
    own_state = pltpu.make_async_copy(state_hbm.at[:, cols(me, width)], state_v.at[cols(me, rows), :], loc.at[1])
    own_state.start()
    pl.semaphore_wait(barrier, n + 1)

    def obs_copy(s):
        peer = flipped(me, s, n)
        return pltpu.make_async_remote_copy(
            src_ref=obs_hbm.at[:, cols(peer, own)], dst_ref=obs_v.at[cols(me, rows), :],
            send_sem=obs_ss.at[s], recv_sem=obs_rs.at[s], device_id=(peer, patch), device_id_type=MESH)

    def state_copy(s):
        peer = flipped(me, s, n)
        return pltpu.make_async_remote_copy(
            src_ref=state_hbm.at[:, cols(peer, width)], dst_ref=state_v.at[cols(me, rows), :],
            send_sem=st_ss.at[s], recv_sem=st_rs.at[s], device_id=(peer, patch), device_id_type=MESH)

    def out_copy(s):
        peer = flipped(me, s, n)
        return pltpu.make_async_remote_copy(
            src_ref=out_v.at[cols(peer, rows), :], dst_ref=out_hbm.at[:, cols(me, width)],
            send_sem=out_ss.at[s], recv_sem=out_rs.at[s], device_id=(peer, patch), device_id_type=MESH)

    for s in steps:
        obs_copy(s).start()
    for s in steps:
        state_copy(s).start()

    own_obs.wait()
    for s in steps:
        obs_copy(s).wait_recv()
    full = obs_v[...].astype(jnp.float32)
    centre = jnp.sum(full, axis=0, keepdims=True) * (1.0 / members)
    root = aux_ref[pl.ds(me, 1), :]
    values = aux_ref[pl.ds(n + me, 1), :]
    own_gain = ((full - centre) * root).astype(jnp.bfloat16)
    innov = (root * (values - centre)).astype(jnp.bfloat16)
    for k in range(2):
        gain[k, pl.ds(0, members), :] = own_gain[:, k * half:(k + 1) * half]
        gain[k, pl.ds(members, PAD), :] = jnp.broadcast_to(
            innov[:, k * half:(k + 1) * half].astype(jnp.float32), (PAD, half)).astype(jnp.bfloat16)

    edges = [
        pltpu.make_async_remote_copy(
            src_ref=gain.at[src], dst_ref=gain.at[dst], send_sem=edge_ss.at[src], recv_sem=edge_rs.at[src],
            device_id=(me, p), device_id_type=MESH)
        for src, dst, p in ((1, 2, up), (0, 3, down))
    ]
    for e in edges:
        e.start()
    for k in range(2):
        gain_t[pl.ds(k * half, half), :] = gain[k, pl.ds(0, members), :].T
    for e in edges:
        e.wait_recv()
    for k in range(2, 4):
        gain_t[pl.ds(k * half, half), :] = gain[k, pl.ds(0, members), :].T

    def gains_of(r0, size):
        return jnp.concatenate([gain[k, pl.ds(r0, size), :] for k in range(4)], axis=1)

    normal = dot(gain_t[...], gains_of(0, members))
    upper = jnp.max(jnp.sum(jnp.abs(normal), axis=0, keepdims=True), axis=1, keepdims=True)
    upper = upper * (1.0 / (members - 1)) + 1e-06
    scaled = normal * (2.0 / (members - 1) / upper)
    d1[...] = scaled.astype(jnp.bfloat16)

    nodes, table = functionals()
    wide = jnp.broadcast_to(upper, (1, nobs))
    f_samples, e_samples = [], []
    for k in range(DEGREE + 1):
        m = wide * float(nodes[k])
        lifted = jnp.sqrt(1.0 + m)
        f_samples.append(-1.0 / (lifted * (1.0 + lifted)))
        e_samples.append(1.0 / (1.0 + m))

    def combined(samples):
        out = []
        for j in range(DEGREE + 1):
            total = samples[0] * float(table[j, 0])
            for k in range(1, DEGREE + 1):
                total = total + samples[k] * float(table[j, k])
            out.append(total)
        return out

    fa = combined(f_samples)
    ea = combined(e_samples)

    t = scaled
    second = 2.0 * dot(d1[...], d1[...]) - 4.0 * t
    d2[...] = second.astype(jnp.bfloat16)
    third = 2.0 * dot(d1[...], d2[...]) + t - 2.0 * second
    d3[...] = third.astype(jnp.bfloat16)
    fourth = 2.0 * dot(d2[...], d2[...]) + 4.0 * second
    d4[...] = fourth.astype(jnp.bfloat16)
    tail = fa[5] * t + fa[6] * second + fa[7] * third
    poly = fa[1] * t + fa[2] * second + fa[3] * third + fa[4] * fourth + dot(d4[...], tail.astype(jnp.bfloat16))

    dvec = jnp.concatenate([gain[k, pl.ds(members, PAD), :] for k in range(4)], axis=1)[0:1, :].astype(jnp.float32)
    y1 = row_times(dvec, d1[...])
    y2 = row_times(dvec, d2[...])
    y3 = row_times(dvec, d3[...])
    w = ea[5] * y1 + ea[6] * y2 + ea[7] * y3
    y4 = row_times(w + ea[4] * dvec, d4[...])
    u = ea[0] * dvec + ea[1] * y1 + ea[2] * y2 + ea[3] * y3 + y4
    poly_b = poly.astype(jnp.bfloat16)

    gsum = jnp.sum(gain_t[...].astype(jnp.float32), axis=1, keepdims=True)
    csum = jnp.zeros((1, width), jnp.float32)
    gr = group * rows
    for i, s in enumerate([0] + order[::-1]):
        base = flipped(me // group, s, groups)
        if s == 0:
            own_state.wait()
        for j in range(group):
            if s * group + j:
                state_copy(s * group + j).wait_recv()
        block = state_v[cols(base, gr), :]
        csum = csum + jnp.sum(block.astype(jnp.float32), axis=0, keepdims=True)
        part = dot(gain_t[:, cols(base, gr)], block)
        if i == 0:
            pt[...] = part
        else:
            pt[...] += part
    product = pt[...] - gsum * (csum * (1.0 / members))
    product_b = product.astype(jnp.bfloat16)
    scale = 1.0 / (members - 1)
    mixed = (fa[0][:, 0:1] * product + dot(poly_b, product_b)) * scale
    d1[...] = mixed.astype(jnp.bfloat16)
    shift = row_times(u, product_b) * scale

    for s in order + [0]:
        base = flipped(me // group, s, groups)
        start = pl.multiple_of(base * gr, gr)
        g = jnp.concatenate([gain[k, pl.ds(start, gr), :] for k in range(4)], axis=1)
        update = dot(g, d1[...])
        out_v[cols(base, gr), :] = (
            state_v[cols(base, gr), :].astype(jnp.float32) + shift + update
        ).astype(jnp.bfloat16)
        for j in range(group):
            if s * group + j:
                out_copy(s * group + j).start()
    keep = pltpu.make_async_copy(out_v.at[cols(me, rows), :], out_hbm.at[:, cols(me, width)], loc.at[2])
    keep.start()

    for e in edges:
        e.wait_send()
    for s in range(1, n):
        obs_copy(s).wait_send()
        state_copy(s).wait_send()
    keep.wait()
    for s in range(1, n):
        out_copy(s).wait()


def on_device(n, npatch, state, obs_ens, obs_values, obs_weight, counts):
    rows = obs_ens.shape[0]
    own = obs_ens.shape[1] // n
    width = state.shape[1] // n
    members = rows * n
    nobs = 2 * own
    mask = (lax.broadcasted_iota(jnp.int32, (n, own), 1) < counts[:, None]).astype(jnp.float32)
    root = jnp.sqrt(obs_weight.reshape(n, own) * mask)
    aux = jnp.concatenate([root, obs_values.reshape(n, own)], axis=0)
    bf, f32 = jnp.bfloat16, jnp.float32
    dma = pltpu.SemaphoreType.DMA
    hbm = pl.BlockSpec(memory_space=pl.ANY)
    return pl.pallas_call(
        functools.partial(kernel, n, npatch),
        out_shape=jax.ShapeDtypeStruct(state.shape, bf),
        in_specs=[pl.BlockSpec(memory_space=pltpu.VMEM), hbm, hbm],
        out_specs=hbm,
        scratch_shapes=[
            pltpu.VMEM((members, own), bf),
            pltpu.VMEM((members, width), bf),
            pltpu.VMEM((4, members + PAD, own // 2), bf),
            pltpu.VMEM((nobs, members), bf),
            pltpu.VMEM((nobs, width), f32),
            pltpu.VMEM((members, width), bf),
            pltpu.VMEM((nobs, nobs), bf),
            pltpu.VMEM((nobs, nobs), bf),
            pltpu.VMEM((nobs, nobs), bf),
            pltpu.VMEM((nobs, nobs), bf),
            dma((n,)), dma((n,)), dma((n,)), dma((n,)),
            dma((2,)), dma((2,)), dma((n,)), dma((n,)), dma((3,)),
        ],
        compiler_params=pltpu.CompilerParams(collective_id=0, has_side_effects=True),
    )(aux, obs_ens, state)


def solution(mesh):
    placed = (P("mem", "patch"), P("mem", "patch"), P("patch"), P("patch"), P("patch"))
    body = functools.partial(on_device, mesh.shape["mem"], mesh.shape["patch"])
    return jax.shard_map(
        body, mesh=mesh, in_specs=placed, out_specs=P("mem", "patch"), check_vma=False
    )
```

```python
import functools
import math

import jax
import jax.numpy as jnp
import numpy as np
from jax import lax
from jax.experimental import pallas as pl
from jax.experimental.pallas import tpu as pltpu
from jax.sharding import PartitionSpec as P

DEGREE = 7
MESH = pl.DeviceIdType.MESH
PAD = 16


def functionals():
    number = DEGREE + 1
    theta = (np.arange(number) + 0.5) * (math.pi / number)
    rows = 2.0 / number * np.cos(np.arange(number)[:, None] * theta[None, :])
    rows[0] *= 0.5
    a = rows
    signs = np.where(np.arange(number) % 2 == 0, 1.0, -1.0)
    table = np.stack(
        [
            (signs[:, None] * a).sum(0),
            a[1] - a[7] + 2 * a[5],
            a[2] + a[6],
            a[3] - a[5] + 2 * a[7],
            a[4] - 2 * a[5] + 2 * a[6] - 2 * a[7],
            2 * a[5],
            2 * a[6],
            2 * a[7],
        ]
    )
    return (np.cos(theta) + 1.0) * 0.5, table


def flipped(index, step, count):
    bit = 1
    while bit < count:
        if step & bit:
            index = index + bit - 2 * bit * (lax.rem(index // bit, 2))
        bit *= 2
    return index


def split(row):
    high = row.astype(jnp.bfloat16)
    low = (row - high.astype(jnp.float32)).astype(jnp.bfloat16)
    return high, low


def row_times(row, matrix):
    high, low = split(row)
    k = row.shape[1]
    pick = lax.broadcasted_iota(jnp.int32, (PAD, k), 0)
    both = jnp.where(
        pick == 0,
        jnp.broadcast_to(high.astype(jnp.float32), (PAD, k)),
        jnp.where(pick == 1, jnp.broadcast_to(low.astype(jnp.float32), (PAD, k)), 0.0),
    ).astype(jnp.bfloat16)
    return jnp.sum(dot(both, matrix), axis=0, keepdims=True)


def dot(left, right):
    return jnp.dot(left, right, preferred_element_type=jnp.float32)


def kernel(
    n, npatch,
    val_hbm, wgt_hbm, cnt_hbm, obs_hbm, state_hbm, out_hbm,
    val_v, wgt_v, cnt_s, side, edge_v, obs_v, state_v, gain, gain_t, pt, out_v,
    d1, d2, d3, d4,
    obs_ss, obs_rs, st_ss, st_rs, edge_ss, edge_rs, side_ss, side_rs, out_ss, out_rs, loc,
):
    me = lax.axis_index("mem")
    patch = lax.axis_index("patch")
    rows = obs_hbm.shape[0]
    own = obs_v.shape[1]
    half = own // 2
    width = state_v.shape[1]
    members = n * rows
    nobs = 2 * own
    up = lax.rem(patch + 1, npatch)
    down = lax.rem(patch + npatch - 1, npatch)

    def cols(index, size):
        return pl.ds(pl.multiple_of(index * size, size), size)

    group = max(1, 256 // rows)
    groups = n // group
    order = list(range(groups - 1, 0, -1))
    steps = [s * group + i for i in range(group) for s in order] + list(range(1, group))

    arrivals = list(range(1, group)) + [s for s in steps if s >= group]

    barrier = pltpu.get_barrier_semaphore()
    for s in range(1, n):
        pl.semaphore_signal(barrier, inc=1, device_id=(flipped(me, s, n), patch), device_id_type=MESH)
    for p in (up, down):
        pl.semaphore_signal(barrier, inc=1, device_id=(me, p), device_id_type=MESH)
    own_obs = pltpu.make_async_copy(obs_hbm.at[:, cols(me, own)], obs_v.at[cols(me, rows), :], loc.at[0])
    own_obs.start()
    own_state = pltpu.make_async_copy(state_hbm.at[:, cols(me, width)], state_v.at[cols(me, rows), :], loc.at[1])
    own_state.start()
    small = [
        pltpu.make_async_copy(src, dst, loc.at[3 + i])
        for i, (src, dst) in enumerate(((val_hbm, val_v), (wgt_hbm, wgt_v), (cnt_hbm, cnt_s)))
    ]
    for c in small:
        c.start()
    pl.semaphore_wait(barrier, n + 1)

    def obs_copy(s):
        peer = flipped(me, s, n)
        return pltpu.make_async_remote_copy(
            src_ref=obs_hbm.at[:, cols(peer, own)], dst_ref=obs_v.at[cols(me, rows), :],
            send_sem=obs_ss.at[s], recv_sem=obs_rs.at[s], device_id=(peer, patch), device_id_type=MESH)

    def state_copy(s):
        peer = flipped(me, s, n)
        return pltpu.make_async_remote_copy(
            src_ref=state_hbm.at[:, cols(peer, width)], dst_ref=state_v.at[cols(me, rows), :],
            send_sem=st_ss.at[s], recv_sem=st_rs.at[s], device_id=(peer, patch), device_id_type=MESH)

    def out_copy(s):
        peer = flipped(me, s, n)
        return pltpu.make_async_remote_copy(
            src_ref=out_v.at[cols(peer, rows), :], dst_ref=out_hbm.at[:, cols(me, width)],
            send_sem=out_ss.at[s], recv_sem=out_rs.at[s], device_id=(peer, patch), device_id_type=MESH)

    for s in steps:
        obs_copy(s).start()
    for s in steps:
        state_copy(s).start()

    def edge_copy(slot, s):
        block = cols(flipped(me, s, n), rows)
        return pltpu.make_async_remote_copy(
            src_ref=obs_v.at[block, pl.ds((1 - slot) * half, half)], dst_ref=edge_v.at[slot, block, :],
            send_sem=edge_ss.at[slot, s], recv_sem=edge_rs.at[slot, s],
            device_id=(me, down if slot else up), device_id_type=MESH)

    def side_copy(slot):
        return pltpu.make_async_remote_copy(
            src_ref=side.at[1 - slot], dst_ref=side.at[2 + slot],
            send_sem=side_ss.at[slot], recv_sem=side_rs.at[slot],
            device_id=(me, down if slot else up), device_id_type=MESH)

    own_obs.wait()
    for slot in range(2):
        edge_copy(slot, 0).start()
    for c in small:
        c.wait()
    count = cnt_s[me]
    for k in range(2):
        lane = lax.broadcasted_iota(jnp.int32, (1, half), 1) + k * half
        mask = jnp.where(lane < count, 1.0, 0.0)
        root = jnp.sqrt(wgt_v[pl.ds(2 * me + k, 1), :] * mask)
        pick = lax.broadcasted_iota(jnp.int32, (8, half), 0)
        side[k] = jnp.where(pick == 0, root, val_v[pl.ds(2 * me + k, 1), :])
    for s in arrivals:
        obs_copy(s).wait_recv()
        for slot in range(2):
            edge_copy(slot, s).start()
    for slot in range(2):
        side_copy(slot).start()

    innovs = [None] * 4

    def perturb(k, block):
        full = block.astype(jnp.float32)
        centre = jnp.sum(full, axis=0, keepdims=True) * (1.0 / members)
        root = side[k, pl.ds(0, 1), :]
        values = side[k, pl.ds(1, 1), :]
        scaled_block = ((full - centre) * root).astype(jnp.bfloat16)
        gain[k] = scaled_block
        gain_t[pl.ds(k * half, half), :] = scaled_block.T
        innovs[k] = (root * (values - centre)).astype(jnp.bfloat16).astype(jnp.float32)

    for k in range(2):
        perturb(k, obs_v[:, k * half:(k + 1) * half])
    for slot in range(2):
        side_copy(slot).wait_recv()
        for s in range(n):
            edge_copy(slot, s).wait_recv()
    for slot in range(2):
        perturb(2 + slot, edge_v[slot])

    def gains_of(r0, size):
        return jnp.concatenate([gain[k, pl.ds(r0, size), :] for k in range(4)], axis=1)

    normal = dot(gain_t[...], gains_of(0, members))
    upper = jnp.max(jnp.sum(jnp.abs(normal), axis=0, keepdims=True), axis=1, keepdims=True)
    upper = upper * (1.0 / (members - 1)) + 1e-06
    scaled = normal * (2.0 / (members - 1) / upper)
    d1[...] = scaled.astype(jnp.bfloat16)

    nodes, table = functionals()
    wide = jnp.broadcast_to(upper, (1, nobs))
    f_samples, e_samples = [], []
    for k in range(DEGREE + 1):
        m = wide * float(nodes[k])
        lifted = jnp.sqrt(1.0 + m)
        f_samples.append(-1.0 / (lifted * (1.0 + lifted)))
        e_samples.append(1.0 / (1.0 + m))

    def combined(samples):
        out = []
        for j in range(DEGREE + 1):
            total = samples[0] * float(table[j, 0])
            for k in range(1, DEGREE + 1):
                total = total + samples[k] * float(table[j, k])
            out.append(total)
        return out

    fa = combined(f_samples)
    ea = combined(e_samples)

    t = scaled
    second = 2.0 * dot(d1[...], d1[...]) - 4.0 * t
    d2[...] = second.astype(jnp.bfloat16)
    third = 2.0 * dot(d1[...], d2[...]) + t - 2.0 * second
    d3[...] = third.astype(jnp.bfloat16)
    fourth = 2.0 * dot(d2[...], d2[...]) + 4.0 * second
    d4[...] = fourth.astype(jnp.bfloat16)
    tail = fa[5] * t + fa[6] * second + fa[7] * third
    poly = fa[1] * t + fa[2] * second + fa[3] * third + fa[4] * fourth + dot(d4[...], tail.astype(jnp.bfloat16))

    dvec = jnp.concatenate(innovs, axis=1)
    y1 = row_times(dvec, d1[...])
    y2 = row_times(dvec, d2[...])
    y3 = row_times(dvec, d3[...])
    w = ea[5] * y1 + ea[6] * y2 + ea[7] * y3
    y4 = row_times(w + ea[4] * dvec, d4[...])
    u = ea[0] * dvec + ea[1] * y1 + ea[2] * y2 + ea[3] * y3 + y4
    poly_b = poly.astype(jnp.bfloat16)

    gsum = jnp.sum(gain_t[...].astype(jnp.float32), axis=1, keepdims=True)
    csum = jnp.zeros((1, width), jnp.float32)
    gr = group * rows
    for i, s in enumerate([0] + order[::-1]):
        base = flipped(me // group, s, groups)
        if s == 0:
            own_state.wait()
        for j in range(group):
            if s * group + j:
                state_copy(s * group + j).wait_recv()
        block = state_v[cols(base, gr), :]
        csum = csum + jnp.sum(block.astype(jnp.float32), axis=0, keepdims=True)
        part = dot(gain_t[:, cols(base, gr)], block)
        if i == 0:
            pt[...] = part
        else:
            pt[...] += part
    product = pt[...] - gsum * (csum * (1.0 / members))
    product_b = product.astype(jnp.bfloat16)
    scale = 1.0 / (members - 1)
    mixed = (fa[0][:, 0:1] * product + dot(poly_b, product_b)) * scale
    d1[...] = mixed.astype(jnp.bfloat16)
    shift = row_times(u, product_b) * scale

    for s in order + [0]:
        base = flipped(me // group, s, groups)
        start = pl.multiple_of(base * gr, gr)
        g = jnp.concatenate([gain[k, pl.ds(start, gr), :] for k in range(4)], axis=1)
        update = dot(g, d1[...])
        out_v[cols(base, gr), :] = (
            state_v[cols(base, gr), :].astype(jnp.float32) + shift + update
        ).astype(jnp.bfloat16)
        for j in range(group):
            if s * group + j:
                out_copy(s * group + j).start()
    keep = pltpu.make_async_copy(out_v.at[cols(me, rows), :], out_hbm.at[:, cols(me, width)], loc.at[2])
    keep.start()

    for slot in range(2):
        side_copy(slot).wait_send()
        for s in range(n):
            edge_copy(slot, s).wait_send()
    for s in range(1, n):
        obs_copy(s).wait_send()
        state_copy(s).wait_send()
    keep.wait()
    for s in range(1, n):
        out_copy(s).wait()


def on_device(n, npatch, state, obs_ens, obs_values, obs_weight, counts):
    rows = obs_ens.shape[0]
    own = obs_ens.shape[1] // n
    width = state.shape[1] // n
    members = rows * n
    nobs = 2 * own
    half = own // 2
    bf, f32 = jnp.bfloat16, jnp.float32
    dma = pltpu.SemaphoreType.DMA
    hbm = pl.BlockSpec(memory_space=pl.ANY)
    return pl.pallas_call(
        functools.partial(kernel, n, npatch),
        out_shape=jax.ShapeDtypeStruct(state.shape, bf),
        in_specs=[pl.BlockSpec(memory_space=pltpu.HBM)] * 5,
        out_specs=hbm,
        scratch_shapes=[
            pltpu.VMEM((2 * n, half), f32),
            pltpu.VMEM((2 * n, half), f32),
            pltpu.SMEM((n,), jnp.int32),
            pltpu.VMEM((4, 8, half), f32),
            pltpu.VMEM((2, members, half), bf),
            pltpu.VMEM((members, own), bf),
            pltpu.VMEM((members, width), bf),
            pltpu.VMEM((4, members, half), bf),
            pltpu.VMEM((nobs, members), bf),
            pltpu.VMEM((nobs, width), f32),
            pltpu.VMEM((members, width), bf),
            pltpu.VMEM((nobs, nobs), bf),
            pltpu.VMEM((nobs, nobs), bf),
            pltpu.VMEM((nobs, nobs), bf),
            pltpu.VMEM((nobs, nobs), bf),
            dma((n,)), dma((n,)), dma((n,)), dma((n,)),
            dma((2, n)), dma((2, n)), dma((2,)), dma((2,)), dma((n,)), dma((n,)), dma((6,)),
        ],
        compiler_params=pltpu.CompilerParams(collective_id=0, has_side_effects=True),
    )(obs_values.reshape(2 * n, half), obs_weight.reshape(2 * n, half), counts, obs_ens, state)


def solution(mesh):
    placed = (P("mem", "patch"), P("mem", "patch"), P("patch"), P("patch"), P("patch"))
    body = functools.partial(on_device, mesh.shape["mem"], mesh.shape["patch"])
    return jax.shard_map(
        body, mesh=mesh, in_specs=placed, out_specs=P("mem", "patch"), check_vma=False
    )
```

```python
import functools
import math

import jax
import jax.numpy as jnp
import numpy as np
from jax import lax
from jax.experimental import pallas as pl
from jax.experimental.pallas import tpu as pltpu
from jax.sharding import PartitionSpec as P

DEGREE = 7
MESH = pl.DeviceIdType.MESH
PAD = 16


def functionals():
    number = DEGREE + 1
    theta = (np.arange(number) + 0.5) * (math.pi / number)
    rows = 2.0 / number * np.cos(np.arange(number)[:, None] * theta[None, :])
    rows[0] *= 0.5
    a = rows
    signs = np.where(np.arange(number) % 2 == 0, 1.0, -1.0)
    table = np.stack(
        [
            (signs[:, None] * a).sum(0),
            a[1] - a[7] + 2 * a[5],
            a[2] + a[6],
            a[3] - a[5] + 2 * a[7],
            a[4] - 2 * a[5] + 2 * a[6] - 2 * a[7],
            2 * a[5],
            2 * a[6],
            2 * a[7],
        ]
    )
    return (np.cos(theta) + 1.0) * 0.5, table


def flipped(index, step, count):
    bit = 1
    while bit < count:
        if step & bit:
            index = index + bit - 2 * bit * (lax.rem(index // bit, 2))
        bit *= 2
    return index


def split(row):
    high = row.astype(jnp.bfloat16)
    low = (row - high.astype(jnp.float32)).astype(jnp.bfloat16)
    return high, low


def row_times(row, matrix):
    high, low = split(row)
    k = row.shape[1]
    pick = lax.broadcasted_iota(jnp.int32, (PAD, k), 0)
    both = jnp.where(
        pick == 0,
        jnp.broadcast_to(high.astype(jnp.float32), (PAD, k)),
        jnp.where(pick == 1, jnp.broadcast_to(low.astype(jnp.float32), (PAD, k)), 0.0),
    ).astype(jnp.bfloat16)
    return jnp.sum(dot(both, matrix), axis=0, keepdims=True)


def dot(left, right):
    return jnp.dot(left, right, preferred_element_type=jnp.float32)


def kernel(
    n, npatch,
    val_hbm, wgt_hbm, cnt_hbm, obs_hbm, state_hbm, out_hbm,
    val_v, wgt_v, cnt_s, side, edge_v, obs_v, state_v, gain, gain_t, pt, out_v,
    d1, d2, d3, d4,
    obs_ss, obs_rs, st_ss, st_rs, edge_ss, edge_rs, side_ss, side_rs, out_ss, out_rs, loc,
):
    me = lax.axis_index("mem")
    patch = lax.axis_index("patch")
    rows = obs_hbm.shape[0]
    own = obs_v.shape[1]
    half = own // 2
    width = state_v.shape[1]
    members = n * rows
    nobs = 2 * own
    up = lax.rem(patch + 1, npatch)
    down = lax.rem(patch + npatch - 1, npatch)

    def cols(index, size):
        return pl.ds(pl.multiple_of(index * size, size), size)

    group = max(1, 256 // rows)
    groups = n // group
    order = list(range(groups - 1, 0, -1))
    steps = [s * group + i for i in range(group) for s in order] + list(range(1, group))

    arrivals = list(range(1, group)) + [s for s in steps if s >= group]

    barrier = pltpu.get_barrier_semaphore()
    for s in range(1, n):
        pl.semaphore_signal(barrier, inc=1, device_id=(flipped(me, s, n), patch), device_id_type=MESH)
    for p in (up, down):
        pl.semaphore_signal(barrier, inc=1, device_id=(me, p), device_id_type=MESH)
    own_obs = pltpu.make_async_copy(obs_hbm.at[:, cols(me, own)], obs_v.at[cols(me, rows), :], loc.at[0])
    own_obs.start()
    own_state = pltpu.make_async_copy(state_hbm.at[:, cols(me, width)], state_v.at[cols(me, rows), :], loc.at[1])
    own_state.start()
    small = [
        pltpu.make_async_copy(src, dst, loc.at[3 + i])
        for i, (src, dst) in enumerate(((val_hbm, val_v), (wgt_hbm, wgt_v), (cnt_hbm, cnt_s)))
    ]
    for c in small:
        c.start()
    pl.semaphore_wait(barrier, n + 1)

    def obs_copy(s):
        peer = flipped(me, s, n)
        return pltpu.make_async_remote_copy(
            src_ref=obs_hbm.at[:, cols(peer, own)], dst_ref=obs_v.at[cols(me, rows), :],
            send_sem=obs_ss.at[s], recv_sem=obs_rs.at[s], device_id=(peer, patch), device_id_type=MESH)

    def state_copy(s):
        peer = flipped(me, s, n)
        return pltpu.make_async_remote_copy(
            src_ref=state_hbm.at[:, cols(peer, width)], dst_ref=state_v.at[cols(me, rows), :],
            send_sem=st_ss.at[s], recv_sem=st_rs.at[s], device_id=(peer, patch), device_id_type=MESH)

    def out_copy(s):
        peer = flipped(me, s, n)
        return pltpu.make_async_remote_copy(
            src_ref=out_v.at[cols(peer, rows), :], dst_ref=out_hbm.at[:, cols(me, width)],
            send_sem=out_ss.at[s], recv_sem=out_rs.at[s], device_id=(peer, patch), device_id_type=MESH)

    for s in steps:
        obs_copy(s).start()
    for s in steps:
        state_copy(s).start()

    def edge_copy(slot, s):
        block = cols(flipped(me, s, n), rows)
        return pltpu.make_async_remote_copy(
            src_ref=obs_v.at[block, pl.ds((1 - slot) * half, half)], dst_ref=edge_v.at[slot, block, :],
            send_sem=edge_ss.at[slot, s], recv_sem=edge_rs.at[slot, s],
            device_id=(me, down if slot else up), device_id_type=MESH)

    def side_copy(slot):
        return pltpu.make_async_remote_copy(
            src_ref=side.at[1 - slot], dst_ref=side.at[2 + slot],
            send_sem=side_ss.at[slot], recv_sem=side_rs.at[slot],
            device_id=(me, down if slot else up), device_id_type=MESH)

    own_obs.wait()
    for slot in range(2):
        edge_copy(slot, 0).start()
    for c in small:
        c.wait()
    count = cnt_s[me]
    for k in range(2):
        lane = lax.broadcasted_iota(jnp.int32, (1, half), 1) + k * half
        mask = jnp.where(lane < count, 1.0, 0.0)
        root = jnp.sqrt(wgt_v[pl.ds(2 * me + k, 1), :] * mask)
        pick = lax.broadcasted_iota(jnp.int32, (8, half), 0)
        side[k] = jnp.where(pick == 0, root, val_v[pl.ds(2 * me + k, 1), :])
    for s in arrivals:
        obs_copy(s).wait_recv()
        for slot in range(2):
            edge_copy(slot, s).start()
    for slot in range(2):
        side_copy(slot).start()

    innovs = [None] * 4

    def perturb(k, block):
        full = block.astype(jnp.float32)
        centre = jnp.sum(full, axis=0, keepdims=True) * (1.0 / members)
        root = side[k, pl.ds(0, 1), :]
        values = side[k, pl.ds(1, 1), :]
        scaled_block = ((full - centre) * root).astype(jnp.bfloat16)
        gain[k] = scaled_block
        gain_t[pl.ds(k * half, half), :] = scaled_block.T
        innovs[k] = (root * (values - centre)).astype(jnp.bfloat16).astype(jnp.float32)

    for k in range(2):
        perturb(k, obs_v[:, k * half:(k + 1) * half])
    for slot in range(2):
        side_copy(slot).wait_recv()
        for s in range(n):
            edge_copy(slot, s).wait_recv()
    for slot in range(2):
        perturb(2 + slot, edge_v[slot])

    def gains_of(r0, size):
        return jnp.concatenate([gain[k, pl.ds(r0, size), :] for k in range(4)], axis=1)

    normal = dot(gain_t[...], gains_of(0, members))
    upper = jnp.max(jnp.sum(jnp.abs(normal), axis=0, keepdims=True), axis=1, keepdims=True)
    upper = upper * (1.0 / (members - 1)) + 1e-06
    scaled = normal * (2.0 / (members - 1) / upper)
    d1[...] = scaled.astype(jnp.bfloat16)

    nodes, table = functionals()
    wide = jnp.broadcast_to(upper, (1, nobs))
    f_samples, e_samples = [], []
    for k in range(DEGREE + 1):
        m = wide * float(nodes[k])
        lifted = jnp.sqrt(1.0 + m)
        f_samples.append(-1.0 / (lifted * (1.0 + lifted)))
        e_samples.append(1.0 / (1.0 + m))

    def combined(samples):
        out = []
        for j in range(DEGREE + 1):
            total = samples[0] * float(table[j, 0])
            for k in range(1, DEGREE + 1):
                total = total + samples[k] * float(table[j, k])
            out.append(total)
        return out

    fa = combined(f_samples)
    ea = combined(e_samples)

    t = scaled
    second = 2.0 * dot(d1[...], d1[...]) - 4.0 * t
    d2[...] = second.astype(jnp.bfloat16)
    third = 2.0 * dot(d1[...], d2[...]) + t - 2.0 * second
    d3[...] = third.astype(jnp.bfloat16)
    fourth = 2.0 * dot(d2[...], d2[...]) + 4.0 * second
    d4[...] = fourth.astype(jnp.bfloat16)
    tail = fa[5] * t + fa[6] * second + fa[7] * third
    poly = fa[1] * t + fa[2] * second + fa[3] * third + fa[4] * fourth + dot(d4[...], tail.astype(jnp.bfloat16))

    dvec = jnp.concatenate(innovs, axis=1)
    y1 = row_times(dvec, d1[...])
    y2 = row_times(dvec, d2[...])
    y3 = row_times(dvec, d3[...])
    w = ea[5] * y1 + ea[6] * y2 + ea[7] * y3
    y4 = row_times(w + ea[4] * dvec, d4[...])
    u = ea[0] * dvec + ea[1] * y1 + ea[2] * y2 + ea[3] * y3 + y4
    poly_b = poly.astype(jnp.bfloat16)

    gsum = jnp.sum(gain_t[...].astype(jnp.float32), axis=1, keepdims=True)
    csum = jnp.zeros((1, width), jnp.float32)
    gr = group * rows
    for i, s in enumerate([0] + order[::-1]):
        base = flipped(me // group, s, groups)
        if s == 0:
            own_state.wait()
        for j in range(group):
            if s * group + j:
                state_copy(s * group + j).wait_recv()
        block = state_v[cols(base, gr), :]
        csum = csum + jnp.sum(block.astype(jnp.float32), axis=0, keepdims=True)
        part = dot(gain_t[:, cols(base, gr)], block)
        if i == 0:
            pt[...] = part
        else:
            pt[...] += part
    product = pt[...] - gsum * (csum * (1.0 / members))
    product_b = product.astype(jnp.bfloat16)
    scale = 1.0 / (members - 1)
    mixed = (fa[0][:, 0:1] * product + dot(poly_b, product_b)) * scale
    d1[...] = mixed.astype(jnp.bfloat16)
    shift = row_times(u, product_b) * scale

    for s in order + [0]:
        base = flipped(me // group, s, groups)
        start = pl.multiple_of(base * gr, gr)
        g = jnp.concatenate([gain[k, pl.ds(start, gr), :] for k in range(4)], axis=1)
        update = dot(g, d1[...])
        out_v[cols(base, gr), :] = (
            state_v[cols(base, gr), :].astype(jnp.float32) + shift + update
        ).astype(jnp.bfloat16)
        for j in range(group):
            if s * group + j:
                out_copy(s * group + j).start()
    keep = pltpu.make_async_copy(out_v.at[cols(me, rows), :], out_hbm.at[:, cols(me, width)], loc.at[2])
    keep.start()

    for slot in range(2):
        side_copy(slot).wait_send()
        for s in range(n):
            edge_copy(slot, s).wait_send()
    for s in range(1, n):
        obs_copy(s).wait_send()
        state_copy(s).wait_send()
    keep.wait()
    for s in range(1, n):
        out_copy(s).wait()


def on_device(n, npatch, state, obs_ens, obs_values, obs_weight, counts):
    rows = obs_ens.shape[0]
    own = obs_ens.shape[1] // n
    width = state.shape[1] // n
    members = rows * n
    nobs = 2 * own
    half = own // 2
    bf, f32 = jnp.bfloat16, jnp.float32
    dma = pltpu.SemaphoreType.DMA
    hbm = pl.BlockSpec(memory_space=pl.ANY)
    return pl.pallas_call(
        functools.partial(kernel, n, npatch),
        out_shape=jax.ShapeDtypeStruct(state.shape, bf),
        in_specs=[pl.BlockSpec(memory_space=pltpu.HBM)] * 5,
        out_specs=hbm,
        scratch_shapes=[
            pltpu.VMEM((2 * n, half), f32),
            pltpu.VMEM((2 * n, half), f32),
            pltpu.SMEM((n,), jnp.int32),
            pltpu.VMEM((4, 8, half), f32),
            pltpu.VMEM((2, members, half), bf),
            pltpu.VMEM((members, own), bf),
            pltpu.VMEM((members, width), bf),
            pltpu.VMEM((4, members, half), bf),
            pltpu.VMEM((nobs, members), bf),
            pltpu.VMEM((nobs, width), f32),
            pltpu.VMEM((members, width), bf),
            pltpu.VMEM((nobs, nobs), bf),
            pltpu.VMEM((nobs, nobs), bf),
            pltpu.VMEM((nobs, nobs), bf),
            pltpu.VMEM((nobs, nobs), bf),
            dma((n,)), dma((n,)), dma((n,)), dma((n,)),
            dma((2, n)), dma((2, n)), dma((2,)), dma((2,)), dma((n,)), dma((n,)), dma((6,)),
        ],
        compiler_params=pltpu.CompilerParams(collective_id=0, has_side_effects=True, vmem_limit_bytes=28 * 1024 * 1024),
    )(*(pltpu.with_memory_space_constraint(x, pltpu.HBM) for x in (obs_values.reshape(2 * n, half), obs_weight.reshape(2 * n, half), counts, obs_ens, state)))


def solution(mesh):
    placed = (P("mem", "patch"), P("mem", "patch"), P("patch"), P("patch"), P("patch"))
    body = functools.partial(on_device, mesh.shape["mem"], mesh.shape["patch"])
    return jax.shard_map(
        body, mesh=mesh, in_specs=placed, out_specs=P("mem", "patch"), check_vma=False
    )
```

```python
import functools
import math

import jax
import jax.numpy as jnp
import numpy as np
from jax import lax
from jax.experimental import pallas as pl
from jax.experimental.pallas import tpu as pltpu
from jax.sharding import PartitionSpec as P

DEGREE = 7
MESH = pl.DeviceIdType.MESH
PAD = 16


def functionals():
    number = DEGREE + 1
    theta = (np.arange(number) + 0.5) * (math.pi / number)
    rows = 2.0 / number * np.cos(np.arange(number)[:, None] * theta[None, :])
    rows[0] *= 0.5
    a = rows
    signs = np.where(np.arange(number) % 2 == 0, 1.0, -1.0)
    table = np.stack(
        [
            (signs[:, None] * a).sum(0),
            a[1] - a[7] + 2 * a[5],
            a[2] + a[6],
            a[3] - a[5] + 2 * a[7],
            a[4] - 2 * a[5] + 2 * a[6] - 2 * a[7],
            2 * a[5],
            2 * a[6],
            2 * a[7],
        ]
    )
    return (np.cos(theta) + 1.0) * 0.5, table


def flipped(index, step, count):
    bit = 1
    while bit < count:
        if step & bit:
            index = index + bit - 2 * bit * (lax.rem(index // bit, 2))
        bit *= 2
    return index


def split(row):
    high = row.astype(jnp.bfloat16)
    low = (row - high.astype(jnp.float32)).astype(jnp.bfloat16)
    return high, low


def row_times(row, matrix):
    high, low = split(row)
    k = row.shape[1]
    pick = lax.broadcasted_iota(jnp.int32, (PAD, k), 0)
    both = jnp.where(
        pick == 0,
        jnp.broadcast_to(high.astype(jnp.float32), (PAD, k)),
        jnp.where(pick == 1, jnp.broadcast_to(low.astype(jnp.float32), (PAD, k)), 0.0),
    ).astype(jnp.bfloat16)
    return jnp.sum(dot(both, matrix), axis=0, keepdims=True)


def dot(left, right):
    return jnp.dot(left, right, preferred_element_type=jnp.float32)


def kernel(
    n, npatch,
    val_hbm, wgt_hbm, cnt_hbm, obs_hbm, state_hbm, out_hbm,
    val_v, wgt_v, cnt_s, side, edge_v, obs_v, state_v, gain, gain_t, pt, out_v,
    d1, d2, d3, d4,
    obs_ss, obs_rs, st_ss, st_rs, edge_ss, edge_rs, side_ss, side_rs, out_ss, out_rs, loc,
):
    me = lax.axis_index("mem")
    patch = lax.axis_index("patch")
    rows = obs_hbm.shape[0]
    own = obs_v.shape[1]
    half = own // 2
    width = state_v.shape[1]
    members = n * rows
    nobs = 2 * own
    up = lax.rem(patch + 1, npatch)
    down = lax.rem(patch + npatch - 1, npatch)

    def cols(index, size):
        return pl.ds(pl.multiple_of(index * size, size), size)

    group = max(1, 256 // rows)
    groups = n // group
    order = list(range(groups - 1, 0, -1))
    steps = [s * group + i for i in range(group) for s in order[::-1]] + list(range(1, group))

    arrivals = list(range(1, group)) + [s for s in steps if s >= group]

    barrier = pltpu.get_barrier_semaphore()
    for s in range(1, n):
        pl.semaphore_signal(barrier, inc=1, device_id=(flipped(me, s, n), patch), device_id_type=MESH)
    for p in (up, down):
        pl.semaphore_signal(barrier, inc=1, device_id=(me, p), device_id_type=MESH)
    own_obs = pltpu.make_async_copy(obs_hbm.at[:, cols(me, own)], obs_v.at[cols(me, rows), :], loc.at[0])
    own_obs.start()
    own_state = pltpu.make_async_copy(state_hbm.at[:, cols(me, width)], state_v.at[cols(me, rows), :], loc.at[1])
    own_state.start()
    small = [
        pltpu.make_async_copy(src, dst, loc.at[3 + i])
        for i, (src, dst) in enumerate(((val_hbm, val_v), (wgt_hbm, wgt_v), (cnt_hbm, cnt_s)))
    ]
    for c in small:
        c.start()
    pl.semaphore_wait(barrier, n + 1)

    def obs_copy(s):
        peer = flipped(me, s, n)
        return pltpu.make_async_remote_copy(
            src_ref=obs_hbm.at[:, cols(peer, own)], dst_ref=obs_v.at[cols(me, rows), :],
            send_sem=obs_ss.at[s], recv_sem=obs_rs.at[s], device_id=(peer, patch), device_id_type=MESH)

    def state_copy(s):
        peer = flipped(me, s, n)
        return pltpu.make_async_remote_copy(
            src_ref=state_hbm.at[:, cols(peer, width)], dst_ref=state_v.at[cols(me, rows), :],
            send_sem=st_ss.at[s], recv_sem=st_rs.at[s], device_id=(peer, patch), device_id_type=MESH)

    def out_copy(s):
        peer = flipped(me, s, n)
        return pltpu.make_async_remote_copy(
            src_ref=out_v.at[cols(peer, rows), :], dst_ref=out_hbm.at[:, cols(me, width)],
            send_sem=out_ss.at[s], recv_sem=out_rs.at[s], device_id=(peer, patch), device_id_type=MESH)

    for s in steps:
        obs_copy(s).start()
    for s in steps:
        state_copy(s).start()

    def edge_copy(slot, s):
        block = cols(flipped(me, s, n), rows)
        return pltpu.make_async_remote_copy(
            src_ref=obs_v.at[block, pl.ds((1 - slot) * half, half)], dst_ref=edge_v.at[slot, block, :],
            send_sem=edge_ss.at[slot, s], recv_sem=edge_rs.at[slot, s],
            device_id=(me, down if slot else up), device_id_type=MESH)

    def side_copy(slot):
        return pltpu.make_async_remote_copy(
            src_ref=side.at[1 - slot], dst_ref=side.at[2 + slot],
            send_sem=side_ss.at[slot], recv_sem=side_rs.at[slot],
            device_id=(me, down if slot else up), device_id_type=MESH)

    own_obs.wait()
    for slot in range(2):
        edge_copy(slot, 0).start()
    for c in small:
        c.wait()
    count = cnt_s[me]
    for k in range(2):
        lane = lax.broadcasted_iota(jnp.int32, (1, half), 1) + k * half
        mask = jnp.where(lane < count, 1.0, 0.0)
        root = jnp.sqrt(wgt_v[pl.ds(2 * me + k, 1), :] * mask)
        pick = lax.broadcasted_iota(jnp.int32, (8, half), 0)
        side[k] = jnp.where(pick == 0, root, val_v[pl.ds(2 * me + k, 1), :])
    for s in arrivals:
        obs_copy(s).wait_recv()
        for slot in range(2):
            edge_copy(slot, s).start()
    for slot in range(2):
        side_copy(slot).start()

    innovs = [None] * 4

    def perturb(k, block):
        full = block.astype(jnp.float32)
        centre = jnp.sum(full, axis=0, keepdims=True) * (1.0 / members)
        root = side[k, pl.ds(0, 1), :]
        values = side[k, pl.ds(1, 1), :]
        scaled_block = ((full - centre) * root).astype(jnp.bfloat16)
        gain[k] = scaled_block
        gain_t[pl.ds(k * half, half), :] = scaled_block.T
        innovs[k] = (root * (values - centre)).astype(jnp.bfloat16).astype(jnp.float32)

    for k in range(2):
        perturb(k, obs_v[:, k * half:(k + 1) * half])
    for slot in range(2):
        side_copy(slot).wait_recv()
        for s in range(n):
            edge_copy(slot, s).wait_recv()
    for slot in range(2):
        perturb(2 + slot, edge_v[slot])

    def gains_of(r0, size):
        return jnp.concatenate([gain[k, pl.ds(r0, size), :] for k in range(4)], axis=1)

    normal = dot(gain_t[...], gains_of(0, members))
    upper = jnp.max(jnp.sum(jnp.abs(normal), axis=0, keepdims=True), axis=1, keepdims=True)
    upper = upper * (1.0 / (members - 1)) + 1e-06
    scaled = normal * (2.0 / (members - 1) / upper)
    d1[...] = scaled.astype(jnp.bfloat16)

    nodes, table = functionals()
    wide = jnp.broadcast_to(upper, (1, nobs))
    f_samples, e_samples = [], []
    for k in range(DEGREE + 1):
        m = wide * float(nodes[k])
        lifted = jnp.sqrt(1.0 + m)
        f_samples.append(-1.0 / (lifted * (1.0 + lifted)))
        e_samples.append(1.0 / (1.0 + m))

    def combined(samples):
        out = []
        for j in range(DEGREE + 1):
            total = samples[0] * float(table[j, 0])
            for k in range(1, DEGREE + 1):
                total = total + samples[k] * float(table[j, k])
            out.append(total)
        return out

    fa = combined(f_samples)
    ea = combined(e_samples)

    t = scaled
    second = 2.0 * dot(d1[...], d1[...]) - 4.0 * t
    d2[...] = second.astype(jnp.bfloat16)
    third = 2.0 * dot(d1[...], d2[...]) + t - 2.0 * second
    d3[...] = third.astype(jnp.bfloat16)
    fourth = 2.0 * dot(d2[...], d2[...]) + 4.0 * second
    d4[...] = fourth.astype(jnp.bfloat16)
    tail = fa[5] * t + fa[6] * second + fa[7] * third
    poly = fa[1] * t + fa[2] * second + fa[3] * third + fa[4] * fourth + dot(d4[...], tail.astype(jnp.bfloat16))

    dvec = jnp.concatenate(innovs, axis=1)
    y1 = row_times(dvec, d1[...])
    y2 = row_times(dvec, d2[...])
    y3 = row_times(dvec, d3[...])
    w = ea[5] * y1 + ea[6] * y2 + ea[7] * y3
    y4 = row_times(w + ea[4] * dvec, d4[...])
    u = ea[0] * dvec + ea[1] * y1 + ea[2] * y2 + ea[3] * y3 + y4
    poly_b = poly.astype(jnp.bfloat16)

    gsum = jnp.sum(gain_t[...].astype(jnp.float32), axis=1, keepdims=True)
    csum = jnp.zeros((1, width), jnp.float32)
    gr = group * rows
    for i, s in enumerate([0] + order[::-1]):
        base = flipped(me // group, s, groups)
        if s == 0:
            own_state.wait()
        for j in range(group):
            if s * group + j:
                state_copy(s * group + j).wait_recv()
        block = state_v[cols(base, gr), :]
        csum = csum + jnp.sum(block.astype(jnp.float32), axis=0, keepdims=True)
        part = dot(gain_t[:, cols(base, gr)], block)
        if i == 0:
            pt[...] = part
        else:
            pt[...] += part
    product = pt[...] - gsum * (csum * (1.0 / members))
    product_b = product.astype(jnp.bfloat16)
    scale = 1.0 / (members - 1)
    mixed = (fa[0][:, 0:1] * product + dot(poly_b, product_b)) * scale
    d1[...] = mixed.astype(jnp.bfloat16)
    shift = row_times(u, product_b) * scale

    for s in order + [0]:
        base = flipped(me // group, s, groups)
        start = pl.multiple_of(base * gr, gr)
        g = jnp.concatenate([gain[k, pl.ds(start, gr), :] for k in range(4)], axis=1)
        update = dot(g, d1[...])
        out_v[cols(base, gr), :] = (
            state_v[cols(base, gr), :].astype(jnp.float32) + shift + update
        ).astype(jnp.bfloat16)
        for j in range(group):
            if s * group + j:
                out_copy(s * group + j).start()
    keep = pltpu.make_async_copy(out_v.at[cols(me, rows), :], out_hbm.at[:, cols(me, width)], loc.at[2])
    keep.start()

    for slot in range(2):
        side_copy(slot).wait_send()
        for s in range(n):
            edge_copy(slot, s).wait_send()
    for s in range(1, n):
        obs_copy(s).wait_send()
        state_copy(s).wait_send()
    keep.wait()
    for s in range(1, n):
        out_copy(s).wait()


def on_device(n, npatch, state, obs_ens, obs_values, obs_weight, counts):
    rows = obs_ens.shape[0]
    own = obs_ens.shape[1] // n
    width = state.shape[1] // n
    members = rows * n
    nobs = 2 * own
    half = own // 2
    bf, f32 = jnp.bfloat16, jnp.float32
    dma = pltpu.SemaphoreType.DMA
    hbm = pl.BlockSpec(memory_space=pl.ANY)
    return pl.pallas_call(
        functools.partial(kernel, n, npatch),
        out_shape=jax.ShapeDtypeStruct(state.shape, bf),
        in_specs=[pl.BlockSpec(memory_space=pltpu.HBM)] * 5,
        out_specs=hbm,
        scratch_shapes=[
            pltpu.VMEM((2 * n, half), f32),
            pltpu.VMEM((2 * n, half), f32),
            pltpu.SMEM((n,), jnp.int32),
            pltpu.VMEM((4, 8, half), f32),
            pltpu.VMEM((2, members, half), bf),
            pltpu.VMEM((members, own), bf),
            pltpu.VMEM((members, width), bf),
            pltpu.VMEM((4, members, half), bf),
            pltpu.VMEM((nobs, members), bf),
            pltpu.VMEM((nobs, width), f32),
            pltpu.VMEM((members, width), bf),
            pltpu.VMEM((nobs, nobs), bf),
            pltpu.VMEM((nobs, nobs), bf),
            pltpu.VMEM((nobs, nobs), bf),
            pltpu.VMEM((nobs, nobs), bf),
            dma((n,)), dma((n,)), dma((n,)), dma((n,)),
            dma((2, n)), dma((2, n)), dma((2,)), dma((2,)), dma((n,)), dma((n,)), dma((6,)),
        ],
        compiler_params=pltpu.CompilerParams(collective_id=0, has_side_effects=True, vmem_limit_bytes=28 * 1024 * 1024),
    )(*(pltpu.with_memory_space_constraint(x, pltpu.HBM) for x in (obs_values.reshape(2 * n, half), obs_weight.reshape(2 * n, half), counts, obs_ens, state)))


def solution(mesh):
    placed = (P("mem", "patch"), P("mem", "patch"), P("patch"), P("patch"), P("patch"))
    body = functools.partial(on_device, mesh.shape["mem"], mesh.shape["patch"])
    return jax.shard_map(
        body, mesh=mesh, in_specs=placed, out_specs=P("mem", "patch"), check_vma=False
    )
```
